32 devices in a mesh: fsdp: 4 (over y, x), tp: 2 (over core), rep: 4 (over z).
Axes of the slice: x: 2, y: 2, z: 4, core: 2. Of those that a mesh axis runs over, the one named last changes fastest.
Arguments:
- tokens: bfloat16 [4096, 5120], P('fsdp', 'rep'), may hold values from -6 to 6
- ref_qkv: bfloat16 [5120, 7168], P(('rep', 'fsdp'), 'tp'), may hold values from -0.078125 to 0.078125
- ref_bias: float32 [7168], P('tp'), may hold values from -9 to 9
- segment_ids: int32 [4, 1024], P('fsdp'), may hold values from 0 to 7, never falling along the last dimension, each value on 1 to 512 neighbouring positions
- policy_key: bfloat16 [5120, 1024], P(('rep', 'fsdp'), 'tp'), may hold values from -0.078125 to 0.078125
Outputs:
- context: bfloat16 [4096, 5120], P(('fsdp', 'rep'), 'tp')
- policy_key_tp: bfloat16 [5120, 1024], P(None, 'tp')
The draws below stay inside these ranges and needn't reach their ends.
All inputs are finite; a program needn't handle non-finite values.
Results may differ from the reference program's by a relative error of at most 0.0093.
Values may be sent and summed in bfloat16 or wider, within the bound.
A program may use at most 128 MiB of HBM per device.

```python
import math
import jax
import jax.numpy as jnp
import numpy as np
from jax import lax

D = 5120
QH = 40
KVH = 8
HD = 128
TOK_DEV = 1024
TOKENS = 4096
N_FSDP = 4


def draw_ref_bias(key, part):
    width = (QH + 2 * KVH) * HD
    return jnp.clip(0.5 * jax.random.normal(key, (width,), jnp.float32), -3.0, 3.0)


def steps_of(own_key, dims, cuts, least, top_value):
    def one(position, parts):
        steps = jax.random.uniform(jax.random.fold_in(jax.random.fold_in(own_key, 6), position), (parts,), jnp.float32, least / len(cuts), top_value / len(cuts))
        return jnp.repeat(jnp.exp(steps), dims[position] // parts).reshape((-1,) + (1,) * (len(dims) - position - 1))

    level = one(*cuts[0])
    for cut in cuts[1:]:
        level = level * one(*cut)
    return level


def profile(amount, total, bound, skew):
    portions = [(1 << 20) // math.isqrt(rank ** skew) + 1 for rank in range(2, amount + 1)]
    spare, counts = total - bound - (amount - 1), [1] * (amount - 1)
    while spare > 0:
        free = [i for i in range(amount - 1) if counts[i] < bound]
        mass, remaining = sum([portions[i] for i in free]), spare
        for i in free:
            extra = min(bound - counts[i], max(1, remaining * portions[i] // mass), spare)
            counts[i] = counts[i] + extra
            spare = spare - extra
    return np.array([bound] + counts)


def ragged(rng, number_of, total, bound, slope):
    if number_of == 2:
        one = jax.random.randint(rng, (), max(1, total - bound), min(bound, total - 1) + 1)
        return jnp.stack([one, total - one])
    tallies = jnp.asarray(profile(number_of, total, bound, slope), jnp.int32)
    pairs = (number_of - 1) // 2
    giver, sink = tallies[1:1 + 2 * pairs:2], tallies[2:2 + 2 * pairs:2]
    room = jnp.minimum(giver - 1, bound - sink)
    shifted = jax.random.randint(jax.random.fold_in(rng, 1), (pairs,), 0, 1 << 20) % (room + 1)
    tallies = tallies.at[1:1 + 2 * pairs:2].set(giver - shifted).at[2:2 + 2 * pairs:2].set(sink + shifted)
    return tallies[jax.random.permutation(jax.random.fold_in(rng, 2), number_of)]


def noise(own_key, extent, spread, most, pieces=(), kind=jnp.bfloat16):
    result = spread * jax.random.normal(own_key, extent, jnp.float32)
    if pieces:
        result = result * steps_of(own_key, extent, pieces, -0.22, 0.18)
    return jnp.clip(result, -most, most).astype(kind)


def setup_inputs(seed: int = 0) -> dict:
    splits = jax.random.split(jax.random.key(seed), 6)
    tokens = noise(splits[0], (TOKENS, D), 1.0, 6.0, ((0, 4), (1, 4)))
    ref_qkv = noise(splits[1], (D, (QH + 2 * KVH) * HD), D ** -0.5, 0.078125, ((0, 16), (1, 2)))
    ref_bias = draw_ref_bias(jax.random.fold_in(splits[5], 71), 0)
    segment_ids = jax.vmap(lambda own: jnp.searchsorted(jnp.cumsum(ragged(own, max(3, TOK_DEV // 128), TOK_DEV, TOK_DEV // 2, 2)), jnp.arange(TOK_DEV), side="right"))(jax.random.split(splits[3], N_FSDP)).reshape((N_FSDP, TOK_DEV)).astype(jnp.int32)
    policy_key = noise(splits[4], (D, KVH * HD), D ** -0.5, 0.078125, ((0, 16), (1, 2)))
    return {"tokens": tokens, "ref_qkv": ref_qkv, "ref_bias": ref_bias, "segment_ids": segment_ids, "policy_key": policy_key}


def positions_of(seg):
    count = seg.shape[0]
    index = jnp.arange(count, dtype=jnp.int32)
    starts = jnp.concatenate([jnp.ones((1,), bool), seg[1:] != seg[:-1]])
    first = lax.cummax(jnp.where(starts, index, 0).astype(jnp.int32), axis=0)
    return (index - first).astype(jnp.int32)

def rotary(values, pos):
    half = values.shape[-1] // 2
    freq = 1000000.0 ** (-2.0 * jnp.arange(half, dtype=jnp.float32) / values.shape[-1])
    angle = pos.astype(jnp.float32)[:, None] * freq[None, :]
    shape = (values.shape[0],) + (1,) * (values.ndim - 2) + (half,)
    cosine = jnp.cos(angle).reshape(shape)
    sine = jnp.sin(angle).reshape(shape)
    first = values[..., :half]
    second = values[..., half:]
    return jnp.concatenate([first * cosine - second * sine, second * cosine + first * sine], axis=-1)

def reference(tokens, ref_qkv, ref_bias, segment_ids, policy_key):
    share = QH // KVH
    proj = jnp.dot(tokens, ref_qkv, preferred_element_type=jnp.float32) + ref_bias[None, :]
    proj = proj.reshape(N_FSDP, TOK_DEV, KVH, share + 2, HD)

    def one_pack(args):
        block, seg = args
        pos = positions_of(seg)
        query = rotary(block[:, :, :share], pos).astype(jnp.bfloat16)
        keys = rotary(block[:, :, share], pos).astype(jnp.bfloat16)
        vals = block[:, :, share + 1].astype(jnp.bfloat16)
        scores = jnp.einsum('qhgd,khd->hgqk', query.astype(jnp.float32), keys.astype(jnp.float32)) / jnp.sqrt(jnp.float32(HD))
        index = jnp.arange(TOK_DEV)
        allowed = (seg[:, None] == seg[None, :]) & (index[None, :] <= index[:, None])
        scores = jnp.where(allowed[None, None], scores, -1e+30)
        top = lax.optimization_barrier(jnp.max(scores, axis=-1, keepdims=True))
        expo = jnp.exp(scores - top)
        weights = (expo / lax.optimization_barrier(jnp.sum(expo, axis=-1, keepdims=True))).astype(jnp.bfloat16)
        ctx = jnp.einsum('hgqk,khd->qhgd', weights.astype(jnp.float32), vals.astype(jnp.float32))
        return ctx.astype(jnp.bfloat16).reshape(TOK_DEV, QH * HD)
    context = lax.map(one_pack, (proj, segment_ids))
    return (context.reshape(TOKENS, QH * HD), policy_key)
```

```python
import jax
import jax.numpy as jnp
from jax import lax
from jax.experimental import pallas as pl
from jax.experimental.pallas import tpu as pltpu
from jax.sharding import PartitionSpec as P
import functools
import math

MESH = pl.DeviceIdType.MESH

QH = 40
KVH = 8
HD = 128


def positions_of(seg):
    count = seg.shape[0]
    index = jnp.arange(count, dtype=jnp.int32)
    starts = jnp.concatenate([jnp.ones((1,), bool), seg[1:] != seg[:-1]])
    first = lax.cummax(jnp.where(starts, index, 0), axis=0)
    return index - first


def rotary(values, pos):
    half = values.shape[-1] // 2
    freq = 1000000.0 ** (-2.0 * jnp.arange(half, dtype=jnp.float32) / values.shape[-1])
    angle = pos.astype(jnp.float32)[:, None] * freq[None, :]
    shape = (values.shape[0],) + (1,) * (values.ndim - 2) + (half,)
    cosine = jnp.cos(angle).reshape(shape)
    sine = jnp.sin(angle).reshape(shape)
    first = values[..., :half]
    second = values[..., half:]
    return jnp.concatenate(
        [first * cosine - second * sine, second * cosine + first * sine], axis=-1
    )


def per_device(tokens, ref_qkv, ref_bias, segment_ids, policy_key):
    share = QH // KVH
    rows = tokens.shape[0]
    columns = ref_qkv.shape[1]
    groups = columns // ((share + 2) * HD)
    replicas = lax.axis_size("rep")
    mine = rows // replicas
    rank = lax.axis_index("rep")
    partial_value = jnp.dot(
        tokens,
        lax.all_gather(ref_qkv, "fsdp", axis=0, tiled=True),
        preferred_element_type=jnp.float32,
    )
    partial_value = partial_value.reshape(rows, groups, share + 2, HD)
    bias = ref_bias.reshape(groups, share + 2, HD)
    seg = segment_ids[0]
    pos = positions_of(seg)
    start = rank * mine
    my_pos = lax.dynamic_slice_in_dim(pos, start, mine, 0)
    summed = lax.psum_scatter(partial_value, "rep", scatter_dimension=0, tiled=True) + bias[None]
    query = rotary(summed[:, :, :share], my_pos).astype(jnp.bfloat16)
    my_keys = rotary(summed[:, :, share], my_pos).astype(jnp.bfloat16)
    my_vals = summed[:, :, share + 1].astype(jnp.bfloat16)
    keys, vals = (
        lax.all_gather(my_keys, "rep", axis=0, tiled=True),
        lax.all_gather(my_vals, "rep", axis=0, tiled=True),
    )
    scores = jnp.einsum(
        "qhgd,khd->hgqk", query, keys, preferred_element_type=jnp.float32
    ) / jnp.sqrt(jnp.float32(HD))
    query_index = start + jnp.arange(mine, dtype=jnp.int32)
    key_index = jnp.arange(rows, dtype=jnp.int32)
    my_seg = lax.dynamic_slice_in_dim(seg, start, mine, 0)
    allowed = (my_seg[:, None] == seg[None, :]) & (key_index[None, :] <= query_index[:, None])
    scores = jnp.where(allowed[None, None], scores, -1e30)
    top = jnp.max(scores, axis=-1, keepdims=True)
    expo = jnp.exp(scores - top)
    weights = (expo / jnp.sum(expo, axis=-1, keepdims=True)).astype(jnp.bfloat16)
    context = jnp.einsum("hgqk,khd->qhgd", weights, vals, preferred_element_type=jnp.float32)
    context = context.astype(jnp.bfloat16).reshape(mine, groups * share * HD)
    inner = lax.all_gather(policy_key, "rep", axis=0, tiled=True)
    outer = lax.all_gather(inner, "fsdp", axis=0, tiled=True)
    blocks = policy_key.shape[0]
    shards = outer.shape[0] // (blocks * replicas)
    whole = (
        outer.reshape(shards, replicas, blocks, outer.shape[1])
        .transpose(1, 0, 2, 3)
        .reshape(outer.shape)
    )
    return (context, whole)


def neighbours():
    f, r, t = lax.axis_index("fsdp"), lax.axis_index("rep"), lax.axis_index("tp")
    ahead = [{"rep": lax.rem(r + k, 4)} for k in range(4)]
    fx = f - lax.rem(f, 2) + 1 - lax.rem(f, 2)
    fy = lax.rem(f + 2, 4)
    return f, r, t, ahead, fx, fy


def greet(devices):
    barrier = pltpu.get_barrier_semaphore()
    for device in devices:
        pl.semaphore_signal(barrier, inc=1, device_id=device, device_id_type=MESH)
    pl.semaphore_wait(barrier, len(devices))


class Copies:
    def __init__(self, send, recv):
        self.send, self.recv, self.made = send, recv, []

    def start(self, src, dst, device):
        n = len(self.made)
        copy = pltpu.make_async_remote_copy(
            src_ref=src, dst_ref=dst, send_sem=self.send.at[n], recv_sem=self.recv.at[n],
            device_id=device, device_id_type=MESH,
        )
        copy.start()
        self.made.append(copy)
        return copy

    def finish(self):
        for copy in self.made:
            copy.wait_send()


N_GATHER = 27


def gather_kernel(tok, w, x, wg, send, recv, local):
    f, r, t, ahead, fx, fy = neighbours()
    to_x, to_y, partner = {"fsdp": fx}, {"fsdp": fy}, {"tp": 1 - t}
    greet([ahead[1], ahead[2], ahead[3], to_x, to_y, partner])
    copies = Copies(send, recv)
    rows, depth = tok.shape
    block, width = wg.shape[2:]
    half, quarter, hb = rows // 2, rows // 4, block // 2
    source = [lax.rem(r + 4 - k, 4) for k in range(4)]

    def cols(rank):
        return pl.ds(pl.multiple_of(rank * width, 128), width)

    def feats(rank):
        return pl.ds(pl.multiple_of(rank * depth, 128), depth)

    def mine(first, count):
        return pl.ds(pl.multiple_of(t * half + first, quarter), count)

    def across(src, k):
        dst = wg.at[source[k], f]
        return copies.start(src, dst, to_x), copies.start(src, dst, to_y)

    def onward(k):
        first, second = pl.ds(0, hb), pl.ds(hb, hb)
        bx, by = passed[k]
        bx.wait_recv()
        a = copies.start(wg.at[source[k], fx, first], wg.at[source[k], fx, first], to_y)
        by.wait_recv()
        b = copies.start(wg.at[source[k], fy, second], wg.at[source[k], fy, second], to_x)
        return a, b

    passed = {0: across(w.at[:, cols(r)], 0)}
    spread = {
        k: copies.start(w.at[:, cols(lax.rem(r + k, 4))], wg.at[r, f], ahead[k])
        for k in (1, 3, 2)
    }
    part = mine(0, half)
    right = copies.start(tok.at[part], x.at[part, feats(r)], ahead[1])
    left = copies.start(tok.at[part], x.at[part, feats(r)], ahead[3])
    own_x = pltpu.make_async_copy(tok, x.at[:, feats(r)], local.at[0])
    own_w = pltpu.make_async_copy(w.at[:, cols(r)], wg.at[r, f], local.at[1])
    own_x.start()
    own_w.start()
    rest = []
    for k in (1, 3):
        spread[k].wait_recv()
        passed[k] = across(wg.at[source[k], f], k)
    rest += onward(0)
    spread[2].wait_recv()
    passed[2] = across(wg.at[source[2], f], 2)
    rest += onward(1)
    from_left, from_right = feats(source[1]), feats(source[3])
    first, second = mine(0, quarter), mine(quarter, quarter)
    right.wait_recv()
    ring_a = copies.start(x.at[first, from_left], x.at[first, from_left], ahead[1])
    rest.append(copies.start(x.at[part, from_left], x.at[part, from_left], partner))
    left.wait_recv()
    ring_b = copies.start(x.at[second, from_right], x.at[second, from_right], ahead[3])
    rest.append(copies.start(x.at[part, from_right], x.at[part, from_right], partner))
    rest += onward(3)
    rest += onward(2)
    far = feats(source[2])
    ring_a.wait_recv()
    rest.append(copies.start(x.at[first, far], x.at[first, far], partner))
    ring_b.wait_recv()
    rest.append(copies.start(x.at[second, far], x.at[second, far], partner))
    for copy in rest:
        copy.wait_recv()
    own_x.wait()
    own_w.wait()
    copies.finish()


def gather(tokens, ref_qkv):
    rows, depth = tokens.shape
    block, columns = ref_qkv.shape
    width = columns // 4
    any_space = pl.BlockSpec(memory_space=pl.ANY)
    x, wg = pl.pallas_call(
        gather_kernel,
        out_shape=(
            jax.ShapeDtypeStruct((rows, depth * 4), tokens.dtype),
            jax.ShapeDtypeStruct((4, 4, block, width), ref_qkv.dtype),
        ),
        in_specs=[pl.BlockSpec(memory_space=pltpu.VMEM)] * 2,
        out_specs=(any_space, any_space),
        scratch_shapes=[
            pltpu.SemaphoreType.DMA((N_GATHER,)),
            pltpu.SemaphoreType.DMA((N_GATHER,)),
            pltpu.SemaphoreType.DMA((2,)),
        ],
        compiler_params=pltpu.CompilerParams(collective_id=0, has_side_effects=True),
        cost_estimate=pl.CostEstimate(flops=0, bytes_accessed=300_000_000, transcendentals=0),
    )(tokens, ref_qkv)
    return x, wg.reshape(16 * block, width)


N_ATTEND = 18


def attend_kernel(proj, bias, cosine, sine, seg_col, seg_row, pol, out, pg, keys, vals, ctx, send, recv, local):
    f, r, t, ahead, fx, fy = neighbours()
    to_x, to_y = {"fsdp": fx}, {"fsdp": fy}
    greet([ahead[1], ahead[2], ahead[3], to_x, to_y])
    copies = Copies(send, recv)
    rows = proj.shape[0]
    mine = rows // 4
    share = proj.shape[1] // HD - 2
    block, width = pol.shape
    hb, hw = block // 2, width // 2
    lo, hi = pl.ds(0, hw), pl.ds(hw, hw)
    top, low = pl.ds(0, hb), pl.ds(hb, hb)
    behind, front, far = lax.rem(r + 3, 4), lax.rem(r + 1, 4), lax.rem(r + 2, 4)

    own_p = pltpu.make_async_copy(pol, pg.at[r, f], local.at[0])
    own_p.start()
    b_x = copies.start(pol.at[:, hi], pg.at[r, f, :, hi], to_x)
    b_y = copies.start(pol.at[:, hi], pg.at[r, f, :, hi], to_y)
    a_z = [copies.start(pol.at[:, lo], pg.at[r, f, :, lo], ahead[k]) for k in (1, 3, 2)]

    def rotated(values, at):
        return values * cosine[at, :] + pltpu.roll(values, HD // 2, 1) * sine[at, :]

    def column(j):
        return pl.ds(pl.multiple_of(j * HD, HD), HD)

    for i in range(4):
        at = pl.ds(i * mine, mine)
        kc, vc = column(share), column(share + 1)
        keys[at, :] = rotated(proj[at, kc] + bias[:, kc], at).astype(jnp.bfloat16)
        vals[at, :] = (proj[at, vc] + bias[:, vc]).astype(jnp.bfloat16)

    span = 3 * mine
    scale = 1.0 / math.sqrt(HD)

    def attend(k):
        d = lax.rem(r + k, 4)
        q0 = pl.multiple_of(d * mine, mine)
        k0 = pl.multiple_of((d // 3) * mine, mine)
        at, window = pl.ds(q0, mine), pl.ds(k0, span)
        q_index = q0 + lax.broadcasted_iota(jnp.int32, (mine, span), 0)
        k_index = k0 + lax.broadcasted_iota(jnp.int32, (mine, span), 1)
        allowed = (seg_col[at, :] == seg_row[:, window]) & (k_index <= q_index)
        shut = jnp.where(allowed, 0.0, -1e30)
        kk, vv = keys[window, :], vals[window, :]

        def head(j, _):
            c = column(j)
            query = rotated(proj[at, c] + bias[:, c], at).astype(jnp.bfloat16)
            scores = lax.dot_general(
                query, kk, (((1,), (1,)), ((), ())), preferred_element_type=jnp.float32
            ) * scale + shut
            expo = jnp.exp(scores - jnp.max(scores, axis=-1, keepdims=True))
            total = jnp.sum(expo, axis=-1, keepdims=True)
            weights = (expo * (1.0 / total)).astype(jnp.bfloat16)
            ctx[k, :, c] = jnp.dot(weights, vv, preferred_element_type=jnp.float32).astype(jnp.bfloat16)
            return 0

        lax.fori_loop(0, share, head, 0)

    place = pl.ds(pl.multiple_of(r * share * HD, HD), share * HD)
    rest = []
    attend(2)
    rest.append(copies.start(ctx.at[2], out.at[:, place], ahead[2]))
    own_p.wait()
    for copy in a_z:
        copy.wait_recv()
    a_x = copies.start(pg.at[:, f, :, lo], pg.at[:, f, :, lo], to_x)
    a_y = copies.start(pg.at[:, f, :, lo], pg.at[:, f, :, lo], to_y)
    b_x.wait_recv()
    b_y.wait_recv()
    d_x = copies.start(pg.at[r, fx, top, hi], pg.at[r, fx, top, hi], to_y)
    d_y = copies.start(pg.at[r, fy, low, hi], pg.at[r, fy, low, hi], to_x)
    attend(1)
    rest.append(copies.start(ctx.at[1], out.at[:, place], ahead[1]))
    attend(3)
    rest.append(copies.start(ctx.at[3], out.at[:, place], ahead[3]))
    d_x.wait_recv()
    d_y.wait_recv()
    z_a = copies.start(pg.at[r, :, :, hi], pg.at[r, :, :, hi], ahead[1])
    z_b = copies.start(pg.at[r, :, :, hi], pg.at[r, :, :, hi], ahead[3])
    attend(0)
    own_c = pltpu.make_async_copy(ctx.at[0], out.at[:, place], local.at[1])
    own_c.start()
    a_x.wait_recv()
    rest.append(copies.start(pg.at[:, fx, top, lo], pg.at[:, fx, top, lo], to_y))
    a_y.wait_recv()
    rest.append(copies.start(pg.at[:, fy, low, lo], pg.at[:, fy, low, lo], to_x))
    z_a.wait_recv()
    rest.append(copies.start(pg.at[behind, pl.ds(0, 2), :, hi], pg.at[behind, pl.ds(0, 2), :, hi], ahead[1]))
    z_b.wait_recv()
    rest.append(copies.start(pg.at[front, pl.ds(2, 2), :, hi], pg.at[front, pl.ds(2, 2), :, hi], ahead[3]))
    for copy in rest:
        copy.wait_recv()
    own_c.wait()
    copies.finish()


def attend_all(proj, bias, cosine, sine, seg, policy_key):
    rows, columns = proj.shape
    mine, share = rows // 4, columns // HD - 2
    block, width = policy_key.shape
    any_space = pl.BlockSpec(memory_space=pl.ANY)
    out, pg = pl.pallas_call(
        attend_kernel,
        out_shape=(
            jax.ShapeDtypeStruct((mine, 4 * share * HD), jnp.bfloat16),
            jax.ShapeDtypeStruct((4, 4, block, width), policy_key.dtype),
        ),
        in_specs=[pl.BlockSpec(memory_space=pltpu.VMEM)] * 7,
        out_specs=(any_space, any_space),
        scratch_shapes=[
            pltpu.VMEM((rows, HD), jnp.bfloat16),
            pltpu.VMEM((rows, HD), jnp.bfloat16),
            pltpu.VMEM((4, mine, share * HD), jnp.bfloat16),
            pltpu.SemaphoreType.DMA((N_ATTEND,)),
            pltpu.SemaphoreType.DMA((N_ATTEND,)),
            pltpu.SemaphoreType.DMA((2,)),
        ],
        compiler_params=pltpu.CompilerParams(collective_id=1, has_side_effects=True),
        cost_estimate=pl.CostEstimate(flops=0, bytes_accessed=150_000_000, transcendentals=0),
    )(proj, bias, cosine, sine, seg[:, None], seg[None, :], policy_key)
    return out, pg.reshape(16 * block, width)


def per_group(tokens, ref_qkv, ref_bias, segment_ids, policy_key):
    rank = lax.axis_index("rep")
    width = ref_qkv.shape[1] // 4
    bias = lax.dynamic_slice_in_dim(ref_bias, rank * width, width, 0)[None, :]
    seg = segment_ids[0]
    pos = positions_of(seg)
    half = HD // 2
    freq = 1000000.0 ** (-2.0 * jnp.arange(half, dtype=jnp.float32) / HD)
    angle = pos.astype(jnp.float32)[:, None] * freq[None, :]
    cosine, sine = jnp.cos(angle), jnp.sin(angle)
    cosine = jnp.concatenate([cosine, cosine], axis=-1)
    sine = jnp.concatenate([-sine, sine], axis=-1)
    x, wg = gather(tokens, ref_qkv)
    proj = jnp.dot(x, wg, preferred_element_type=jnp.float32)
    return attend_all(proj, bias, cosine, sine, seg, policy_key)


def solution(mesh):
    in_specs = (
        P("fsdp", "rep"),
        P(("rep", "fsdp"), "tp"),
        P("tp"),
        P("fsdp", None),
        P(("rep", "fsdp"), "tp"),
    )
    out_specs = (P(("fsdp", "rep"), "tp"), P(None, "tp"))
    shape = mesh.shape
    grouped = (
        shape["rep"] == 4 and shape["fsdp"] == 4 and shape["tp"] == 2 and KVH == shape["tp"] * shape["rep"]
    )
    return jax.shard_map(
        per_group if grouped else per_device, mesh=mesh, in_specs=in_specs, out_specs=out_specs, check_vma=False
    )
```

```python
import jax
import jax.numpy as jnp
from jax import lax
from jax.experimental import pallas as pl
from jax.experimental.pallas import tpu as pltpu
from jax.sharding import PartitionSpec as P
import functools
import math

MESH = pl.DeviceIdType.MESH

QH = 40
KVH = 8
HD = 128


def positions_of(seg):
    count = seg.shape[0]
    index = jnp.arange(count, dtype=jnp.int32)
    starts = jnp.concatenate([jnp.ones((1,), bool), seg[1:] != seg[:-1]])
    first = lax.cummax(jnp.where(starts, index, 0), axis=0)
    return index - first


def rotary(values, pos):
    half = values.shape[-1] // 2
    freq = 1000000.0 ** (-2.0 * jnp.arange(half, dtype=jnp.float32) / values.shape[-1])
    angle = pos.astype(jnp.float32)[:, None] * freq[None, :]
    shape = (values.shape[0],) + (1,) * (values.ndim - 2) + (half,)
    cosine = jnp.cos(angle).reshape(shape)
    sine = jnp.sin(angle).reshape(shape)
    first = values[..., :half]
    second = values[..., half:]
    return jnp.concatenate(
        [first * cosine - second * sine, second * cosine + first * sine], axis=-1
    )


def per_device(tokens, ref_qkv, ref_bias, segment_ids, policy_key):
    share = QH // KVH
    rows = tokens.shape[0]
    columns = ref_qkv.shape[1]
    groups = columns // ((share + 2) * HD)
    replicas = lax.axis_size("rep")
    mine = rows // replicas
    rank = lax.axis_index("rep")
    partial_value = jnp.dot(
        tokens,
        lax.all_gather(ref_qkv, "fsdp", axis=0, tiled=True),
        preferred_element_type=jnp.float32,
    )
    partial_value = partial_value.reshape(rows, groups, share + 2, HD)
    bias = ref_bias.reshape(groups, share + 2, HD)
    seg = segment_ids[0]
    pos = positions_of(seg)
    start = rank * mine
    my_pos = lax.dynamic_slice_in_dim(pos, start, mine, 0)
    summed = lax.psum_scatter(partial_value, "rep", scatter_dimension=0, tiled=True) + bias[None]
    query = rotary(summed[:, :, :share], my_pos).astype(jnp.bfloat16)
    my_keys = rotary(summed[:, :, share], my_pos).astype(jnp.bfloat16)
    my_vals = summed[:, :, share + 1].astype(jnp.bfloat16)
    keys, vals = (
        lax.all_gather(my_keys, "rep", axis=0, tiled=True),
        lax.all_gather(my_vals, "rep", axis=0, tiled=True),
    )
    scores = jnp.einsum(
        "qhgd,khd->hgqk", query, keys, preferred_element_type=jnp.float32
    ) / jnp.sqrt(jnp.float32(HD))
    query_index = start + jnp.arange(mine, dtype=jnp.int32)
    key_index = jnp.arange(rows, dtype=jnp.int32)
    my_seg = lax.dynamic_slice_in_dim(seg, start, mine, 0)
    allowed = (my_seg[:, None] == seg[None, :]) & (key_index[None, :] <= query_index[:, None])
    scores = jnp.where(allowed[None, None], scores, -1e30)
    top = jnp.max(scores, axis=-1, keepdims=True)
    expo = jnp.exp(scores - top)
    weights = (expo / jnp.sum(expo, axis=-1, keepdims=True)).astype(jnp.bfloat16)
    context = jnp.einsum("hgqk,khd->qhgd", weights, vals, preferred_element_type=jnp.float32)
    context = context.astype(jnp.bfloat16).reshape(mine, groups * share * HD)
    inner = lax.all_gather(policy_key, "rep", axis=0, tiled=True)
    outer = lax.all_gather(inner, "fsdp", axis=0, tiled=True)
    blocks = policy_key.shape[0]
    shards = outer.shape[0] // (blocks * replicas)
    whole = (
        outer.reshape(shards, replicas, blocks, outer.shape[1])
        .transpose(1, 0, 2, 3)
        .reshape(outer.shape)
    )
    return (context, whole)


def neighbours():
    f, r, t = lax.axis_index("fsdp"), lax.axis_index("rep"), lax.axis_index("tp")
    ahead = [{"rep": lax.rem(r + k, 4)} for k in range(4)]
    fx = f - lax.rem(f, 2) + 1 - lax.rem(f, 2)
    fy = lax.rem(f + 2, 4)
    return f, r, t, ahead, fx, fy


def greet(devices):
    barrier = pltpu.get_barrier_semaphore()
    for device in devices:
        pl.semaphore_signal(barrier, inc=1, device_id=device, device_id_type=MESH)
    pl.semaphore_wait(barrier, len(devices))


class Copies:
    def __init__(self, send, recv):
        self.send, self.recv, self.made = send, recv, []

    def start(self, src, dst, device, sends=None):
        n = len(self.made)
        copy = pltpu.make_async_remote_copy(
            src_ref=src, dst_ref=dst, send_sem=self.send.at[n], recv_sem=self.recv.at[n],
            device_id=device, device_id_type=MESH,
        )
        only(sends, copy.start)
        self.made.append((copy, sends))
        return copy

    def finish(self):
        for copy, sends in self.made:
            only(sends, copy.wait_send)


def only(condition, act):
    if condition is None:
        act()
    else:
        pl.when(condition)(act)


N_COPIES = 48


def layer_kernel(
    tok, w, bias, cosine, sine, seg_col, seg_row, pol, out, pg,
    x, wg, proj, keys, vals, ctx, send, recv, local,
):
    f, r, t, ahead, fx, fy = neighbours()
    to_x, to_y, partner = {"fsdp": fx}, {"fsdp": fy}, {"tp": 1 - t}
    greet([ahead[1], ahead[2], ahead[3], to_x, to_y, partner])
    copies = Copies(send, recv)
    rows, depth = tok.shape
    mine, half = rows // 4, rows // 2
    block, width = w.shape[0], wg.shape[2]
    hb = block // 2
    share = width // HD - 2
    pw = pol.shape[1] // 2
    lo, hi = pl.ds(0, pw), pl.ds(pw, pw)
    top, low = pl.ds(0, hb), pl.ds(hb, hb)
    source = [lax.rem(r + 4 - k, 4) for k in range(4)]

    def cols(rank):
        return pl.ds(pl.multiple_of(rank * width, 128), width)

    def held(k, owner, first, count):
        return wg.at[source[k], pl.ds(pl.multiple_of(owner * block + first, 16), count)]

    def across(src, k):
        dst = held(k, f, 0, block)
        return copies.start(src, dst, to_x), copies.start(src, dst, to_y)

    def onward(k):
        bx, by = passed[k]
        bx.wait_recv()
        a = copies.start(held(k, fx, 0, hb), held(k, fx, 0, hb), to_y)
        by.wait_recv()
        b = copies.start(held(k, fy, hb, hb), held(k, fy, hb, hb), to_x)
        return [a, b]

    def policy_z(c):
        return [copies.start(pol.at[:, c], pg.at[r, f, :, c], ahead[k]) for k in (1, 3, 2)]

    def policy_xy(c, arrived):
        for copy in arrived:
            copy.wait_recv()
        src = pg.at[:, f, :, c]
        return copies.start(src, src, to_x), copies.start(src, src, to_y)

    def policy_last(c, pair):
        a, b = pg.at[:, fx, top, c], pg.at[:, fy, low, c]
        pair[0].wait_recv()
        one = copies.start(a, a, to_y)
        pair[1].wait_recv()
        return [one, copies.start(b, b, to_x)]

    part = pl.ds(pl.multiple_of(t * half, half), half)

    def line(k):
        below, above = source[k - 1], lax.rem(r + k - 1, 4)
        up_src = tok.at[part] if k == 1 else x.at[below, part]
        down_src = tok.at[part] if k == 1 else x.at[above, part]
        up = copies.start(up_src, x.at[below, part], ahead[1], (r <= 2) & (r >= k - 1))
        down = copies.start(down_src, x.at[above, part], ahead[3], (r >= 1) & (r <= 4 - k))
        return up, down

    def landed(k, pair):
        only(r >= k, pair[0].wait_recv)
        only(r <= 3 - k, pair[1].wait_recv)

    def to_partner(k):
        below, above = x.at[source[k], part], x.at[lax.rem(r + k, 4), part]
        return (
            copies.start(below, below, partner, r >= k),
            copies.start(above, above, partner, r <= 3 - k),
        )

    def add(left, plane):
        def tile(i, _):
            at = pl.ds(pl.multiple_of(i * mine, mine), mine)
            proj[at, :] += jnp.dot(left[at, :], wg[plane], preferred_element_type=jnp.float32)
            return 0

        lax.fori_loop(0, 4, tile, 0)

    def add_planes(k, pair):
        def below():
            pair[0].wait_recv()
            add(x.at[source[k]], source[k])

        def above():
            pair[1].wait_recv()
            add(x.at[lax.rem(r + k, 4)], lax.rem(r + k, 4))

        only(r >= k, below)
        only(r <= 3 - k, above)

    own_w = pltpu.make_async_copy(w.at[:, cols(r)], held(0, f, 0, block), local.at[0])
    own_p = pltpu.make_async_copy(pol, pg.at[r, f], local.at[1])
    passed = {0: across(w.at[:, cols(r)], 0)}
    spread = {
        k: copies.start(w.at[:, cols(lax.rem(r + k, 4))], wg.at[r, pl.ds(pl.multiple_of(f * block, 16), block)], ahead[k])
        for k in (1, 3, 2)
    }
    lo_z = policy_z(lo)
    line1 = line(1)
    own_w.start()
    own_p.start()
    proj[...] = jnp.broadcast_to(bias[...], proj.shape)
    for k in (1, 3):
        spread[k].wait_recv()
        passed[k] = across(held(k, f, 0, block), k)
    weights_in = onward(0)
    spread[2].wait_recv()
    passed[2] = across(held(2, f, 0, block), 2)
    weights_in += onward(1)
    own_p.wait()
    lo_xy = policy_xy(lo, lo_z)
    weights_in += onward(3)
    landed(1, line1)
    line2 = line(2)
    near = to_partner(1)
    weights_in += onward(2)
    own_w.wait()
    for copy in weights_in[:2]:
        copy.wait_recv()
    add(tok, r)
    for copy in weights_in[2:]:
        copy.wait_recv()
    landed(2, line2)
    line3 = line(3)
    mid = to_partner(2)
    hi_z = policy_z(hi)
    add_planes(1, near)
    rest = policy_last(lo, lo_xy)
    add_planes(2, mid)
    landed(3, line3)
    add_planes(3, to_partner(3))
    hi_xy = policy_xy(hi, hi_z)

    def rotated(values, at):
        return values * cosine[at, :] + pltpu.roll(values, HD // 2, 1) * sine[at, :]

    def column(j):
        return pl.ds(pl.multiple_of(j * HD, HD), HD)

    for i in range(4):
        at = pl.ds(i * mine, mine)
        keys[at, :] = rotated(proj[at, column(share)], at).astype(jnp.bfloat16)
        vals[at, :] = proj[at, column(share + 1)].astype(jnp.bfloat16)

    span = 3 * mine
    scale = 1.0 / math.sqrt(HD)

    def attend(k):
        d = lax.rem(r + k, 4)
        q0 = pl.multiple_of(d * mine, mine)
        k0 = pl.multiple_of((d // 3) * mine, mine)
        at, window = pl.ds(q0, mine), pl.ds(k0, span)
        q_index = q0 + lax.broadcasted_iota(jnp.int32, (mine, span), 0)
        k_index = k0 + lax.broadcasted_iota(jnp.int32, (mine, span), 1)
        allowed = (seg_col[at, :] == seg_row[:, window]) & (k_index <= q_index)
        shut = jnp.where(allowed, 0.0, -1e30)
        kk, vv = keys[window, :], vals[window, :]

        def head(j, _):
            c = column(j)
            query = rotated(proj[at, c], at).astype(jnp.bfloat16)
            scores = lax.dot_general(
                query, kk, (((1,), (1,)), ((), ())), preferred_element_type=jnp.float32
            ) * scale + shut
            expo = jnp.exp(scores - jnp.max(scores, axis=-1, keepdims=True))
            total = jnp.sum(expo, axis=-1, keepdims=True)
            weights = (expo * (1.0 / total)).astype(jnp.bfloat16)
            ctx[k, :, c] = jnp.dot(weights, vv, preferred_element_type=jnp.float32).astype(jnp.bfloat16)
            return 0

        lax.fori_loop(0, share, head, 0)

    place = pl.ds(pl.multiple_of(r * share * HD, HD), share * HD)
    for k in (2, 1, 3):
        attend(k)
        rest.append(copies.start(ctx.at[k], out.at[:, place], ahead[k]))
    attend(0)
    own_c = pltpu.make_async_copy(ctx.at[0], out.at[:, place], local.at[2])
    own_c.start()
    rest += policy_last(hi, hi_xy)
    for copy in rest:
        copy.wait_recv()
    own_c.wait()
    copies.finish()


def whole_layer(tokens, ref_qkv, bias, cosine, sine, seg, policy_key):
    rows, depth = tokens.shape
    block, columns = ref_qkv.shape
    width = columns // 4
    mine, share = rows // 4, width // HD - 2
    any_space = pl.BlockSpec(memory_space=pl.ANY)
    out, pg = pl.pallas_call(
        layer_kernel,
        out_shape=(
            jax.ShapeDtypeStruct((mine, 4 * share * HD), jnp.bfloat16),
            jax.ShapeDtypeStruct((4, 4) + policy_key.shape, policy_key.dtype),
        ),
        in_specs=[pl.BlockSpec(memory_space=pltpu.VMEM)] * 8,
        out_specs=(any_space, any_space),
        scratch_shapes=[
            pltpu.VMEM((4, rows, depth), tokens.dtype),
            pltpu.VMEM((4, 4 * block, width), ref_qkv.dtype),
            pltpu.VMEM((rows, width), jnp.float32),
            pltpu.VMEM((rows, HD), jnp.bfloat16),
            pltpu.VMEM((rows, HD), jnp.bfloat16),
            pltpu.VMEM((4, mine, share * HD), jnp.bfloat16),
            pltpu.SemaphoreType.DMA((N_COPIES,)),
            pltpu.SemaphoreType.DMA((N_COPIES,)),
            pltpu.SemaphoreType.DMA((3,)),
        ],
        compiler_params=pltpu.CompilerParams(
            collective_id=0, has_side_effects=True, vmem_limit_bytes=60 * 1024 * 1024
        ),
    )(tokens, ref_qkv, bias, cosine, sine, seg[:, None], seg[None, :], policy_key)
    return out, pg.reshape((-1,) + policy_key.shape[1:])


def per_group(tokens, ref_qkv, ref_bias, segment_ids, policy_key):
    rank = lax.axis_index("rep")
    width = ref_qkv.shape[1] // 4
    bias = lax.dynamic_slice_in_dim(ref_bias, rank * width, width, 0)[None, :]
    seg = segment_ids[0]
    pos = positions_of(seg)
    half = HD // 2
    freq = 1000000.0 ** (-2.0 * jnp.arange(half, dtype=jnp.float32) / HD)
    angle = pos.astype(jnp.float32)[:, None] * freq[None, :]
    cosine, sine = jnp.cos(angle), jnp.sin(angle)
    cosine = jnp.concatenate([cosine, cosine], axis=-1)
    sine = jnp.concatenate([-sine, sine], axis=-1)
    return whole_layer(tokens, ref_qkv, bias, cosine, sine, seg, policy_key)


def solution(mesh):
    in_specs = (
        P("fsdp", "rep"),
        P(("rep", "fsdp"), "tp"),
        P("tp"),
        P("fsdp", None),
        P(("rep", "fsdp"), "tp"),
    )
    out_specs = (P(("fsdp", "rep"), "tp"), P(None, "tp"))
    shape = mesh.shape
    grouped = (
        shape["rep"] == 4 and shape["fsdp"] == 4 and shape["tp"] == 2 and KVH == shape["tp"] * shape["rep"]
    )
    return jax.shard_map(
        per_group if grouped else per_device, mesh=mesh, in_specs=in_specs, out_specs=out_specs, check_vma=False
    )
```

```python
import jax
import jax.numpy as jnp
from jax import lax
from jax.experimental import pallas as pl
from jax.experimental.pallas import tpu as pltpu
from jax.sharding import PartitionSpec as P
import functools
import math

MESH = pl.DeviceIdType.MESH

QH = 40
KVH = 8
HD = 128


def positions_of(seg):
    count = seg.shape[0]
    index = jnp.arange(count, dtype=jnp.int32)
    starts = jnp.concatenate([jnp.ones((1,), bool), seg[1:] != seg[:-1]])
    first = lax.cummax(jnp.where(starts, index, 0), axis=0)
    return index - first


def rotary(values, pos):
    half = values.shape[-1] // 2
    freq = 1000000.0 ** (-2.0 * jnp.arange(half, dtype=jnp.float32) / values.shape[-1])
    angle = pos.astype(jnp.float32)[:, None] * freq[None, :]
    shape = (values.shape[0],) + (1,) * (values.ndim - 2) + (half,)
    cosine = jnp.cos(angle).reshape(shape)
    sine = jnp.sin(angle).reshape(shape)
    first = values[..., :half]
    second = values[..., half:]
    return jnp.concatenate(
        [first * cosine - second * sine, second * cosine + first * sine], axis=-1
    )


def per_device(tokens, ref_qkv, ref_bias, segment_ids, policy_key):
    share = QH // KVH
    rows = tokens.shape[0]
    columns = ref_qkv.shape[1]
    groups = columns // ((share + 2) * HD)
    replicas = lax.axis_size("rep")
    mine = rows // replicas
    rank = lax.axis_index("rep")
    partial_value = jnp.dot(
        tokens,
        lax.all_gather(ref_qkv, "fsdp", axis=0, tiled=True),
        preferred_element_type=jnp.float32,
    )
    partial_value = partial_value.reshape(rows, groups, share + 2, HD)
    bias = ref_bias.reshape(groups, share + 2, HD)
    seg = segment_ids[0]
    pos = positions_of(seg)
    start = rank * mine
    my_pos = lax.dynamic_slice_in_dim(pos, start, mine, 0)
    summed = lax.psum_scatter(partial_value, "rep", scatter_dimension=0, tiled=True) + bias[None]
    query = rotary(summed[:, :, :share], my_pos).astype(jnp.bfloat16)
    my_keys = rotary(summed[:, :, share], my_pos).astype(jnp.bfloat16)
    my_vals = summed[:, :, share + 1].astype(jnp.bfloat16)
    keys, vals = (
        lax.all_gather(my_keys, "rep", axis=0, tiled=True),
        lax.all_gather(my_vals, "rep", axis=0, tiled=True),
    )
    scores = jnp.einsum(
        "qhgd,khd->hgqk", query, keys, preferred_element_type=jnp.float32
    ) / jnp.sqrt(jnp.float32(HD))
    query_index = start + jnp.arange(mine, dtype=jnp.int32)
    key_index = jnp.arange(rows, dtype=jnp.int32)
    my_seg = lax.dynamic_slice_in_dim(seg, start, mine, 0)
    allowed = (my_seg[:, None] == seg[None, :]) & (key_index[None, :] <= query_index[:, None])
    scores = jnp.where(allowed[None, None], scores, -1e30)
    top = jnp.max(scores, axis=-1, keepdims=True)
    expo = jnp.exp(scores - top)
    weights = (expo / jnp.sum(expo, axis=-1, keepdims=True)).astype(jnp.bfloat16)
    context = jnp.einsum("hgqk,khd->qhgd", weights, vals, preferred_element_type=jnp.float32)
    context = context.astype(jnp.bfloat16).reshape(mine, groups * share * HD)
    inner = lax.all_gather(policy_key, "rep", axis=0, tiled=True)
    outer = lax.all_gather(inner, "fsdp", axis=0, tiled=True)
    blocks = policy_key.shape[0]
    shards = outer.shape[0] // (blocks * replicas)
    whole = (
        outer.reshape(shards, replicas, blocks, outer.shape[1])
        .transpose(1, 0, 2, 3)
        .reshape(outer.shape)
    )
    return (context, whole)


def neighbours():
    f, r, t = lax.axis_index("fsdp"), lax.axis_index("rep"), lax.axis_index("tp")
    ahead = [{"rep": lax.rem(r + k, 4)} for k in range(4)]
    fx = f - lax.rem(f, 2) + 1 - lax.rem(f, 2)
    fy = lax.rem(f + 2, 4)
    return f, r, t, ahead, fx, fy


def greet(devices):
    barrier = pltpu.get_barrier_semaphore()
    for device in devices:
        pl.semaphore_signal(barrier, inc=1, device_id=device, device_id_type=MESH)
    pl.semaphore_wait(barrier, len(devices))


class Copies:
    def __init__(self, send, recv):
        self.send, self.recv, self.made = send, recv, []

    def start(self, src, dst, device, sends=None):
        n = len(self.made)
        copy = pltpu.make_async_remote_copy(
            src_ref=src, dst_ref=dst, send_sem=self.send.at[n], recv_sem=self.recv.at[n],
            device_id=device, device_id_type=MESH,
        )
        only(sends, copy.start)
        self.made.append((copy, sends))
        return copy

    def finish(self):
        for copy, sends in self.made:
            only(sends, copy.wait_send)


def only(condition, act):
    if condition is None:
        act()
    else:
        pl.when(condition)(act)


N_COPIES = 57


def layer_kernel(
    tok, w, bias, cosine, sine, seg_col, seg_row, pol, out, pg,
    x, wg, proj, keys, vals, ctx, send, recv, local, ctx_send, ctx_recv,
):
    f, r, t, ahead, fx, fy = neighbours()
    to_x, to_y, partner = {"fsdp": fx}, {"fsdp": fy}, {"tp": 1 - t}
    greet([ahead[1], ahead[2], ahead[3], to_x, to_y, partner])
    copies = Copies(send, recv)
    rows, depth = tok.shape
    mine, half = rows // 4, rows // 2
    block, width = w.shape[0], wg.shape[2]
    hb = block // 2
    share = width // HD - 2
    pw = pol.shape[1] // 2
    lo, hi = pl.ds(0, pw), pl.ds(pw, pw)
    top, low = pl.ds(0, hb), pl.ds(hb, hb)
    source = [lax.rem(r + 4 - k, 4) for k in range(4)]

    def cols(rank):
        return pl.ds(pl.multiple_of(rank * width, 128), width)

    def held(k, owner, first, count):
        return wg.at[source[k], pl.ds(pl.multiple_of(owner * block + first, 16), count)]

    def across(src, k):
        dst = held(k, f, 0, block)
        return copies.start(src, dst, to_x), copies.start(src, dst, to_y)

    def onward(k):
        bx, by = passed[k]
        bx.wait_recv()
        a = copies.start(held(k, fx, 0, hb), held(k, fx, 0, hb), to_y)
        by.wait_recv()
        b = copies.start(held(k, fy, hb, hb), held(k, fy, hb, hb), to_x)
        return [a, b]

    def policy_z(c):
        return [copies.start(pol.at[:, c], pg.at[r, f, :, c], ahead[k]) for k in (1, 3, 2)]

    def policy_xy(c, arrived):
        for copy in arrived:
            copy.wait_recv()
        src = pg.at[:, f, :, c]
        return copies.start(src, src, to_x), copies.start(src, src, to_y)

    def policy_last(c, pair):
        a, b = pg.at[:, fx, top, c], pg.at[:, fy, low, c]
        pair[0].wait_recv()
        one = copies.start(a, a, to_y)
        pair[1].wait_recv()
        return [one, copies.start(b, b, to_x)]

    parts = [pl.ds(pl.multiple_of(c * half + t * mine, mine), mine) for c in range(2)]

    def line(k, c):
        part = parts[c]
        below, above = source[k - 1], lax.rem(r + k - 1, 4)
        up_src = tok.at[part] if k == 1 else x.at[below, part]
        down_src = tok.at[part] if k == 1 else x.at[above, part]
        up = copies.start(up_src, x.at[below, part], ahead[1], (r <= 2) & (r >= k - 1))
        down = copies.start(down_src, x.at[above, part], ahead[3], (r >= 1) & (r <= 4 - k))
        return up, down

    def landed(k, pair):
        only(r >= k, pair[0].wait_recv)
        only(r <= 3 - k, pair[1].wait_recv)

    def to_partner(k, c):
        part = parts[c]
        below, above = x.at[source[k], part], x.at[lax.rem(r + k, 4), part]
        return (
            copies.start(below, below, partner, r >= k),
            copies.start(above, above, partner, r <= 3 - k),
        )

    def add(left, plane, c):
        def tile(i, _):
            at = pl.ds(pl.multiple_of(c * half + i * mine, mine), mine)
            proj[at, :] += jnp.dot(left[at, :], wg[plane], preferred_element_type=jnp.float32)
            return 0

        lax.fori_loop(0, 2, tile, 0)

    def add_planes(k, pair, c):
        def below():
            pair[0].wait_recv()
            add(x.at[source[k]], source[k], c)

        def above():
            pair[1].wait_recv()
            add(x.at[lax.rem(r + k, 4)], lax.rem(r + k, 4), c)

        only(r >= k, below)
        only(r <= 3 - k, above)

    own_w = pltpu.make_async_copy(w.at[:, cols(r)], held(0, f, 0, block), local.at[0])
    own_p = pltpu.make_async_copy(pol, pg.at[r, f], local.at[1])
    passed = {0: across(w.at[:, cols(r)], 0)}
    spread = {
        k: copies.start(w.at[:, cols(lax.rem(r + k, 4))], wg.at[r, pl.ds(pl.multiple_of(f * block, 16), block)], ahead[k])
        for k in (1, 3, 2)
    }
    lo_z = policy_z(lo)
    near = line(1, 0)
    own_w.start()
    own_p.start()
    proj[...] = jnp.broadcast_to(bias[...], proj.shape)
    for k in (1, 3):
        spread[k].wait_recv()
        passed[k] = across(held(k, f, 0, block), k)
    weights_in = onward(0)
    spread[2].wait_recv()
    passed[2] = across(held(2, f, 0, block), 2)
    weights_in += onward(1)
    own_p.wait()
    lo_xy = policy_xy(lo, lo_z)
    weights_in += onward(3)
    landed(1, near)
    mid = line(2, 0)
    near_late = line(1, 1)
    shared_near = to_partner(1, 0)
    weights_in += onward(2)
    own_w.wait()
    for copy in weights_in[:2]:
        copy.wait_recv()
    add(tok, r, 0)
    landed(2, mid)
    far = line(3, 0)
    shared_mid = to_partner(2, 0)
    landed(1, near_late)
    mid_late = line(2, 1)
    shared_near_late = to_partner(1, 1)
    add(tok, r, 1)
    for copy in weights_in[2:]:
        copy.wait_recv()
    add_planes(1, shared_near, 0)
    rest = policy_last(lo, lo_xy)
    add_planes(2, shared_mid, 0)
    landed(3, far)
    shared_far = to_partner(3, 0)
    landed(2, mid_late)
    far_late = line(3, 1)
    shared_mid_late = to_partner(2, 1)
    hi_z = policy_z(hi)
    add_planes(3, shared_far, 0)

    def rotated(values, at):
        return values * cosine[at, :] + pltpu.roll(values, HD // 2, 1) * sine[at, :]

    def column(j):
        return pl.ds(pl.multiple_of(j * HD, HD), HD)

    scale = 1.0 / math.sqrt(HD)

    def rotate_keys(i):
        at = pl.ds(i * mine, mine)
        keys[at, :] = rotated(proj[at, column(share)], at).astype(jnp.bfloat16)
        vals[at, :] = proj[at, column(share + 1)].astype(jnp.bfloat16)

    place = pl.ds(pl.multiple_of(r * share * HD, HD), share * HD)
    own_c = pltpu.make_async_copy(ctx.at[r], out.at[:, place], local.at[2])

    def send_context(d, step):
        return pltpu.make_async_remote_copy(
            src_ref=ctx.at[d], dst_ref=out.at[:, place],
            send_sem=ctx_send.at[step], recv_sem=ctx_recv.at[step],
            device_id={"rep": d}, device_id_type=MESH,
        )

    def attend(d):
        first = max(d - 2, 0)
        q0, k0, span = d * mine, first * mine, (d + 1 - first) * mine
        at, window = pl.ds(q0, mine), pl.ds(k0, span)
        q_index = q0 + lax.broadcasted_iota(jnp.int32, (mine, span), 0)
        k_index = k0 + lax.broadcasted_iota(jnp.int32, (mine, span), 1)
        allowed = (seg_col[at, :] == seg_row[:, window]) & (k_index <= q_index)
        shut = jnp.where(allowed, 0.0, -1e30)
        kk, vv = keys[window, :], vals[window, :]

        def head(j, _):
            c = column(j)
            query = rotated(proj[at, c], at).astype(jnp.bfloat16)
            scores = lax.dot_general(
                query, kk, (((1,), (1,)), ((), ())), preferred_element_type=jnp.float32
            ) * scale + shut
            expo = jnp.exp(scores - jnp.max(scores, axis=-1, keepdims=True))
            total = jnp.sum(expo, axis=-1, keepdims=True)
            weights = (expo * (1.0 / total)).astype(jnp.bfloat16)
            ctx[d, :, c] = jnp.dot(weights, vv, preferred_element_type=jnp.float32).astype(jnp.bfloat16)
            return 0

        lax.fori_loop(0, share, head, 0)

        pl.when(r == d)(own_c.start)
        pl.when(r != d)(send_context(d, lax.rem(d + 4 - r, 4)).start)

    rotate_keys(0)
    attend(0)
    rotate_keys(1)
    attend(1)
    add_planes(1, shared_near_late, 1)
    add_planes(2, shared_mid_late, 1)
    landed(3, far_late)
    add_planes(3, to_partner(3, 1), 1)
    rotate_keys(2)
    rotate_keys(3)
    attend(3)
    attend(2)
    hi_xy = policy_xy(hi, hi_z)
    rest += policy_last(hi, hi_xy)
    for copy in rest:
        copy.wait_recv()
    own_c.wait()
    for k in (1, 2, 3):
        copy = send_context(lax.rem(r + k, 4), k)
        copy.wait_send()
        copy.wait_recv()
    copies.finish()


def whole_layer(tokens, ref_qkv, bias, cosine, sine, seg, policy_key):
    rows, depth = tokens.shape
    block, columns = ref_qkv.shape
    width = columns // 4
    mine, share = rows // 4, width // HD - 2
    any_space = pl.BlockSpec(memory_space=pl.ANY)
    out, pg = pl.pallas_call(
        layer_kernel,
        out_shape=(
            jax.ShapeDtypeStruct((mine, 4 * share * HD), jnp.bfloat16),
            jax.ShapeDtypeStruct((4, 4) + policy_key.shape, policy_key.dtype),
        ),
        in_specs=[pl.BlockSpec(memory_space=pltpu.VMEM)] * 8,
        out_specs=(any_space, any_space),
        scratch_shapes=[
            pltpu.VMEM((4, rows, depth), tokens.dtype),
            pltpu.VMEM((4, 4 * block, width), ref_qkv.dtype),
            pltpu.VMEM((rows, width), jnp.float32),
            pltpu.VMEM((rows, HD), jnp.bfloat16),
            pltpu.VMEM((rows, HD), jnp.bfloat16),
            pltpu.VMEM((4, mine, share * HD), jnp.bfloat16),
            pltpu.SemaphoreType.DMA((N_COPIES,)),
            pltpu.SemaphoreType.DMA((N_COPIES,)),
            pltpu.SemaphoreType.DMA((3,)),
            pltpu.SemaphoreType.DMA((4,)),
            pltpu.SemaphoreType.DMA((4,)),
        ],
        compiler_params=pltpu.CompilerParams(
            collective_id=0, has_side_effects=True, vmem_limit_bytes=60 * 1024 * 1024
        ),
    )(tokens, ref_qkv, bias, cosine, sine, seg[:, None], seg[None, :], policy_key)
    return out, pg.reshape((-1,) + policy_key.shape[1:])


def per_group(tokens, ref_qkv, ref_bias, segment_ids, policy_key):
    rank = lax.axis_index("rep")
    width = ref_qkv.shape[1] // 4
    bias = lax.dynamic_slice_in_dim(ref_bias, rank * width, width, 0)[None, :]
    seg = segment_ids[0]
    pos = positions_of(seg)
    half = HD // 2
    freq = 1000000.0 ** (-2.0 * jnp.arange(half, dtype=jnp.float32) / HD)
    angle = pos.astype(jnp.float32)[:, None] * freq[None, :]
    cosine, sine = jnp.cos(angle), jnp.sin(angle)
    cosine = jnp.concatenate([cosine, cosine], axis=-1)
    sine = jnp.concatenate([-sine, sine], axis=-1)
    return whole_layer(tokens, ref_qkv, bias, cosine, sine, seg, policy_key)


def solution(mesh):
    in_specs = (
        P("fsdp", "rep"),
        P(("rep", "fsdp"), "tp"),
        P("tp"),
        P("fsdp", None),
        P(("rep", "fsdp"), "tp"),
    )
    out_specs = (P(("fsdp", "rep"), "tp"), P(None, "tp"))
    shape = mesh.shape
    grouped = (
        shape["rep"] == 4 and shape["fsdp"] == 4 and shape["tp"] == 2 and KVH == shape["tp"] * shape["rep"]
    )
    return jax.shard_map(
        per_group if grouped else per_device, mesh=mesh, in_specs=in_specs, out_specs=out_specs, check_vma=False
    )
```

```python
import jax
import jax.numpy as jnp
from jax import lax
from jax.experimental import pallas as pl
from jax.experimental.pallas import tpu as pltpu
from jax.sharding import PartitionSpec as P
import functools
import math

MESH = pl.DeviceIdType.MESH

QH = 40
KVH = 8
HD = 128


def positions_of(seg):
    count = seg.shape[0]
    index = jnp.arange(count, dtype=jnp.int32)
    starts = jnp.concatenate([jnp.ones((1,), bool), seg[1:] != seg[:-1]])
    first = lax.cummax(jnp.where(starts, index, 0), axis=0)
    return index - first


def rotary(values, pos):
    half = values.shape[-1] // 2
    freq = 1000000.0 ** (-2.0 * jnp.arange(half, dtype=jnp.float32) / values.shape[-1])
    angle = pos.astype(jnp.float32)[:, None] * freq[None, :]
    shape = (values.shape[0],) + (1,) * (values.ndim - 2) + (half,)
    cosine = jnp.cos(angle).reshape(shape)
    sine = jnp.sin(angle).reshape(shape)
    first = values[..., :half]
    second = values[..., half:]
    return jnp.concatenate(
        [first * cosine - second * sine, second * cosine + first * sine], axis=-1
    )


def per_device(tokens, ref_qkv, ref_bias, segment_ids, policy_key):
    share = QH // KVH
    rows = tokens.shape[0]
    columns = ref_qkv.shape[1]
    groups = columns // ((share + 2) * HD)
    replicas = lax.axis_size("rep")
    mine = rows // replicas
    rank = lax.axis_index("rep")
    partial_value = jnp.dot(
        tokens,
        lax.all_gather(ref_qkv, "fsdp", axis=0, tiled=True),
        preferred_element_type=jnp.float32,
    )
    partial_value = partial_value.reshape(rows, groups, share + 2, HD)
    bias = ref_bias.reshape(groups, share + 2, HD)
    seg = segment_ids[0]
    pos = positions_of(seg)
    start = rank * mine
    my_pos = lax.dynamic_slice_in_dim(pos, start, mine, 0)
    summed = lax.psum_scatter(partial_value, "rep", scatter_dimension=0, tiled=True) + bias[None]
    query = rotary(summed[:, :, :share], my_pos).astype(jnp.bfloat16)
    my_keys = rotary(summed[:, :, share], my_pos).astype(jnp.bfloat16)
    my_vals = summed[:, :, share + 1].astype(jnp.bfloat16)
    keys, vals = (
        lax.all_gather(my_keys, "rep", axis=0, tiled=True),
        lax.all_gather(my_vals, "rep", axis=0, tiled=True),
    )
    scores = jnp.einsum(
        "qhgd,khd->hgqk", query, keys, preferred_element_type=jnp.float32
    ) / jnp.sqrt(jnp.float32(HD))
    query_index = start + jnp.arange(mine, dtype=jnp.int32)
    key_index = jnp.arange(rows, dtype=jnp.int32)
    my_seg = lax.dynamic_slice_in_dim(seg, start, mine, 0)
    allowed = (my_seg[:, None] == seg[None, :]) & (key_index[None, :] <= query_index[:, None])
    scores = jnp.where(allowed[None, None], scores, -1e30)
    top = jnp.max(scores, axis=-1, keepdims=True)
    expo = jnp.exp(scores - top)
    weights = (expo / jnp.sum(expo, axis=-1, keepdims=True)).astype(jnp.bfloat16)
    context = jnp.einsum("hgqk,khd->qhgd", weights, vals, preferred_element_type=jnp.float32)
    context = context.astype(jnp.bfloat16).reshape(mine, groups * share * HD)
    inner = lax.all_gather(policy_key, "rep", axis=0, tiled=True)
    outer = lax.all_gather(inner, "fsdp", axis=0, tiled=True)
    blocks = policy_key.shape[0]
    shards = outer.shape[0] // (blocks * replicas)
    whole = (
        outer.reshape(shards, replicas, blocks, outer.shape[1])
        .transpose(1, 0, 2, 3)
        .reshape(outer.shape)
    )
    return (context, whole)


def neighbours():
    f, r, t = lax.axis_index("fsdp"), lax.axis_index("rep"), lax.axis_index("tp")
    ahead = [{"rep": lax.rem(r + k, 4)} for k in range(4)]
    fx = f - lax.rem(f, 2) + 1 - lax.rem(f, 2)
    fy = lax.rem(f + 2, 4)
    return f, r, t, ahead, fx, fy


def greet(devices):
    barrier = pltpu.get_barrier_semaphore()
    for device in devices:
        pl.semaphore_signal(barrier, inc=1, device_id=device, device_id_type=MESH)
    pl.semaphore_wait(barrier, len(devices))


class Copies:
    def __init__(self, send, recv):
        self.send, self.recv, self.made = send, recv, []

    def start(self, src, dst, device, sends=None):
        n = len(self.made)
        copy = pltpu.make_async_remote_copy(
            src_ref=src, dst_ref=dst, send_sem=self.send.at[n], recv_sem=self.recv.at[n],
            device_id=device, device_id_type=MESH,
        )
        only(sends, copy.start)
        self.made.append((copy, sends))
        return copy

    def finish(self):
        for copy, sends in self.made:
            only(sends, copy.wait_send)


def only(condition, act):
    if condition is None:
        act()
    else:
        pl.when(condition)(act)


N_COPIES = 57


def layer_kernel(
    tok, w, bias, cosine, sine, seg_col, seg_row, pol, out, pg,
    x, wg, proj, keys, vals, ctx, send, recv, local, ctx_send, ctx_recv,
):
    f, r, t, ahead, fx, fy = neighbours()
    to_x, to_y, partner = {"fsdp": fx}, {"fsdp": fy}, {"tp": 1 - t}
    greet([ahead[1], ahead[2], ahead[3], to_x, to_y, partner])
    copies = Copies(send, recv)
    rows, depth = tok.shape
    mine, half = rows // 4, rows // 2
    block, width = w.shape[0], wg.shape[2]
    hb = block // 2
    share = width // HD - 2
    pw = pol.shape[1] // 2
    lo, hi = pl.ds(0, pw), pl.ds(pw, pw)
    top, low = pl.ds(0, hb), pl.ds(hb, hb)
    source = [lax.rem(r + 4 - k, 4) for k in range(4)]

    def cols(rank):
        return pl.ds(pl.multiple_of(rank * width, 128), width)

    def held(k, owner, first, count):
        return wg.at[source[k], pl.ds(pl.multiple_of(owner * block + first, 16), count)]

    def across(src, k):
        dst = held(k, f, 0, block)
        return copies.start(src, dst, to_x), copies.start(src, dst, to_y)

    def onward(k):
        bx, by = passed[k]
        bx.wait_recv()
        a = copies.start(held(k, fx, 0, hb), held(k, fx, 0, hb), to_y)
        by.wait_recv()
        b = copies.start(held(k, fy, hb, hb), held(k, fy, hb, hb), to_x)
        return [a, b]

    def policy_z(c):
        return [copies.start(pol.at[:, c], pg.at[r, f, :, c], ahead[k]) for k in (1, 3, 2)]

    def policy_xy(c, arrived):
        for copy in arrived:
            copy.wait_recv()
        src = pg.at[:, f, :, c]
        return copies.start(src, src, to_x), copies.start(src, src, to_y)

    def policy_last(c, pair):
        a, b = pg.at[:, fx, top, c], pg.at[:, fy, low, c]
        pair[0].wait_recv()
        one = copies.start(a, a, to_y)
        pair[1].wait_recv()
        return [one, copies.start(b, b, to_x)]

    parts = [pl.ds(pl.multiple_of(c * half + t * mine, mine), mine) for c in range(2)]

    def line(k, c):
        part = parts[c]
        below, above = source[k - 1], lax.rem(r + k - 1, 4)
        up_src = tok.at[part] if k == 1 else x.at[below, part]
        down_src = tok.at[part] if k == 1 else x.at[above, part]
        up = copies.start(up_src, x.at[below, part], ahead[1], (r <= 2) & (r >= k - 1))
        down = copies.start(down_src, x.at[above, part], ahead[3], (r >= 1) & (r <= 4 - k))
        return up, down

    def landed(k, pair):
        only(r >= k, pair[0].wait_recv)
        only(r <= 3 - k, pair[1].wait_recv)

    def to_partner(k, c):
        part = parts[c]
        below, above = x.at[source[k], part], x.at[lax.rem(r + k, 4), part]
        return (
            copies.start(below, below, partner, r >= k),
            copies.start(above, above, partner, r <= 3 - k),
        )

    def add(left, plane, c):
        def tile(i, _):
            at = pl.ds(pl.multiple_of(c * half + i * mine, mine), mine)
            proj[at, :] += jnp.dot(left[at, :], wg[plane], preferred_element_type=jnp.float32)
            return 0

        lax.fori_loop(0, 2, tile, 0)

    def add_planes(k, pair, c):
        def below():
            pair[0].wait_recv()
            add(x.at[source[k]], source[k], c)

        def above():
            pair[1].wait_recv()
            add(x.at[lax.rem(r + k, 4)], lax.rem(r + k, 4), c)

        only(r >= k, below)
        only(r <= 3 - k, above)

    own_w = pltpu.make_async_copy(w.at[:, cols(r)], held(0, f, 0, block), local.at[0])
    own_p = pltpu.make_async_copy(pol, pg.at[r, f], local.at[1])
    passed = {0: across(w.at[:, cols(r)], 0)}
    spread = {
        k: copies.start(w.at[:, cols(lax.rem(r + k, 4))], wg.at[r, pl.ds(pl.multiple_of(f * block, 16), block)], ahead[k])
        for k in (1, 3, 2)
    }
    lo_z = policy_z(lo)
    hi_z = policy_z(hi)
    near = line(1, 0)
    near_late = line(1, 1)
    own_w.start()
    own_p.start()
    proj[...] = jnp.broadcast_to(bias[...], proj.shape)
    for k in (1, 3):
        spread[k].wait_recv()
        passed[k] = across(held(k, f, 0, block), k)
    weights_in = onward(0)
    spread[2].wait_recv()
    passed[2] = across(held(2, f, 0, block), 2)
    weights_in += onward(1)
    weights_in += onward(3)
    landed(1, near)
    mid = line(2, 0)
    shared_near = to_partner(1, 0)
    weights_in += onward(2)
    own_p.wait()
    lo_xy = policy_xy(lo, lo_z)
    hi_xy = policy_xy(hi, hi_z)
    own_w.wait()
    for copy in weights_in[:2]:
        copy.wait_recv()
    landed(1, near_late)
    mid_late = line(2, 1)
    shared_near_late = to_partner(1, 1)
    add(tok, r, 0)
    add(tok, r, 1)
    landed(2, mid)
    far = line(3, 0)
    shared_mid = to_partner(2, 0)
    for copy in weights_in[2:]:
        copy.wait_recv()
    add_planes(1, shared_near, 0)
    rest = policy_last(lo, lo_xy)
    add_planes(2, shared_mid, 0)
    landed(2, mid_late)
    far_late = line(3, 1)
    shared_mid_late = to_partner(2, 1)
    add_planes(1, shared_near_late, 1)
    rest += policy_last(hi, hi_xy)
    landed(3, far)
    add_planes(3, to_partner(3, 0), 0)

    def rotated(values, at):
        return values * cosine[at, :] + pltpu.roll(values, HD // 2, 1) * sine[at, :]

    def column(j):
        return pl.ds(pl.multiple_of(j * HD, HD), HD)

    scale = 1.0 / math.sqrt(HD)

    def rotate_keys(i):
        at = pl.ds(i * mine, mine)
        keys[at, :] = rotated(proj[at, column(share)], at).astype(jnp.bfloat16)
        vals[at, :] = proj[at, column(share + 1)].astype(jnp.bfloat16)

    place = pl.ds(pl.multiple_of(r * share * HD, HD), share * HD)
    own_c = pltpu.make_async_copy(ctx.at[r], out.at[:, place], local.at[2])

    def send_context(d, step):
        return pltpu.make_async_remote_copy(
            src_ref=ctx.at[d], dst_ref=out.at[:, place],
            send_sem=ctx_send.at[step], recv_sem=ctx_recv.at[step],
            device_id={"rep": d}, device_id_type=MESH,
        )

    def attend(d):
        first = max(d - 2, 0)
        q0, k0, span = d * mine, first * mine, (d + 1 - first) * mine
        at, window = pl.ds(q0, mine), pl.ds(k0, span)
        q_index = q0 + lax.broadcasted_iota(jnp.int32, (mine, span), 0)
        k_index = k0 + lax.broadcasted_iota(jnp.int32, (mine, span), 1)
        allowed = (seg_col[at, :] == seg_row[:, window]) & (k_index <= q_index)
        shut = jnp.where(allowed, 0.0, -1e30)
        kk, vv = keys[window, :], vals[window, :]

        def head(j, _):
            c = column(j)
            query = rotated(proj[at, c], at).astype(jnp.bfloat16)
            scores = lax.dot_general(
                query, kk, (((1,), (1,)), ((), ())), preferred_element_type=jnp.float32
            ) * scale + shut
            expo = jnp.exp(scores - jnp.max(scores, axis=-1, keepdims=True))
            total = jnp.sum(expo, axis=-1, keepdims=True)
            weights = (expo * (1.0 / total)).astype(jnp.bfloat16)
            ctx[d, :, c] = jnp.dot(weights, vv, preferred_element_type=jnp.float32).astype(jnp.bfloat16)
            return 0

        lax.fori_loop(0, share, head, 0)

        pl.when(r == d)(own_c.start)
        pl.when(r != d)(send_context(d, lax.rem(d + 4 - r, 4)).start)

    rotate_keys(0)
    attend(0)
    rotate_keys(1)
    attend(1)
    add_planes(2, shared_mid_late, 1)
    landed(3, far_late)
    add_planes(3, to_partner(3, 1), 1)
    rotate_keys(2)
    rotate_keys(3)
    attend(3)
    attend(2)
    for copy in rest:
        copy.wait_recv()
    own_c.wait()
    for k in (1, 2, 3):
        copy = send_context(lax.rem(r + k, 4), k)
        copy.wait_send()
        copy.wait_recv()
    copies.finish()


def whole_layer(tokens, ref_qkv, bias, cosine, sine, seg, policy_key):
    rows, depth = tokens.shape
    block, columns = ref_qkv.shape
    width = columns // 4
    mine, share = rows // 4, width // HD - 2
    any_space = pl.BlockSpec(memory_space=pl.ANY)
    out, pg = pl.pallas_call(
        layer_kernel,
        out_shape=(
            jax.ShapeDtypeStruct((mine, 4 * share * HD), jnp.bfloat16),
            jax.ShapeDtypeStruct((4, 4) + policy_key.shape, policy_key.dtype),
        ),
        in_specs=[pl.BlockSpec(memory_space=pltpu.VMEM)] * 8,
        out_specs=(any_space, any_space),
        scratch_shapes=[
            pltpu.VMEM((4, rows, depth), tokens.dtype),
            pltpu.VMEM((4, 4 * block, width), ref_qkv.dtype),
            pltpu.VMEM((rows, width), jnp.float32),
            pltpu.VMEM((rows, HD), jnp.bfloat16),
            pltpu.VMEM((rows, HD), jnp.bfloat16),
            pltpu.VMEM((4, mine, share * HD), jnp.bfloat16),
            pltpu.SemaphoreType.DMA((N_COPIES,)),
            pltpu.SemaphoreType.DMA((N_COPIES,)),
            pltpu.SemaphoreType.DMA((3,)),
            pltpu.SemaphoreType.DMA((4,)),
            pltpu.SemaphoreType.DMA((4,)),
        ],
        compiler_params=pltpu.CompilerParams(
            collective_id=0, has_side_effects=True, vmem_limit_bytes=60 * 1024 * 1024
        ),
    )(tokens, ref_qkv, bias, cosine, sine, seg[:, None], seg[None, :], policy_key)
    return out, pg.reshape((-1,) + policy_key.shape[1:])


def per_group(tokens, ref_qkv, ref_bias, segment_ids, policy_key):
    rank = lax.axis_index("rep")
    width = ref_qkv.shape[1] // 4
    bias = lax.dynamic_slice_in_dim(ref_bias, rank * width, width, 0)[None, :]
    seg = segment_ids[0]
    pos = positions_of(seg)
    half = HD // 2
    freq = 1000000.0 ** (-2.0 * jnp.arange(half, dtype=jnp.float32) / HD)
    angle = pos.astype(jnp.float32)[:, None] * freq[None, :]
    cosine, sine = jnp.cos(angle), jnp.sin(angle)
    cosine = jnp.concatenate([cosine, cosine], axis=-1)
    sine = jnp.concatenate([-sine, sine], axis=-1)
    return whole_layer(tokens, ref_qkv, bias, cosine, sine, seg, policy_key)


def solution(mesh):
    in_specs = (
        P("fsdp", "rep"),
        P(("rep", "fsdp"), "tp"),
        P("tp"),
        P("fsdp", None),
        P(("rep", "fsdp"), "tp"),
    )
    out_specs = (P(("fsdp", "rep"), "tp"), P(None, "tp"))
    shape = mesh.shape
    grouped = (
        shape["rep"] == 4 and shape["fsdp"] == 4 and shape["tp"] == 2 and KVH == shape["tp"] * shape["rep"]
    )
    return jax.shard_map(
        per_group if grouped else per_device, mesh=mesh, in_specs=in_specs, out_specs=out_specs, check_vma=False
    )
```
